32 devices in a mesh: gx: 4 (over z), yz: 8 (over y, x, core).
Axes of the slice: x: 2, y: 2, z: 4, core: 2. Of those that a mesh axis runs over, the one named last changes fastest.
Arguments:
- brick_ids: int32 [4096, 1], P(('gx', 'yz')), may hold values from 0 to 31; in each aligned block of 128 rows (0 to 127, 128 to 255, ...) at most 4 rows name the same one
- voxel_offset: int32 [4096, 256], P(('gx', 'yz')), may hold values from 0 to 4095
- fractions: float32 [4096, 3, 256], P(('gx', 'yz')), may hold values from 0 to 1
- normals: float32 [4096, 3, 256], P(('gx', 'yz')), may hold values from -6 to 6
- point_weight: float32 [4096, 256], P(('gx', 'yz')), may hold values from 0.1 to 10
- tile_count: int32 [32], P(('gx', 'yz')), may hold values from 96 to 128, as said below
Outputs:
- rhs: float32 [16, 64, 128], P('gx', 'yz')
- screen: float32 [16, 64, 128], P('gx', 'yz')
The draws below stay inside these ranges and needn't reach their ends.
Inputs may be any that keep to these rules, and one draw needn't show every extreme that they name: `brick_ids`: brick b belongs to index b // 8 of gx and b % 8 of yz. Among the 128 tile slots of one device no brick is named more than 4 times. `tile_count`: some device has all its slots valid in every draw.
All inputs are finite; a program needn't handle non-finite values.
Results may differ from the reference program's by a relative error of at most 0.0039.
Values sent between devices are 32-bit elements; how exact they have to be, the bound alone decides.
A program may use at most 64 MiB of HBM per device.

```python
import math
import jax
import jax.numpy as jnp
import numpy as np
from jax import lax

BX = 4
BY = 8
BZ = 128
TILE = 256
TILES_DEV = 128
CAP = 4
TILES = 4096
NX = 16
NY = 64
NZ = 128
N_YZ = 8
DEVICES = 32


def draw_tile_count(key, part):
    first = jax.random.fold_in(key, 11)
    second = jax.random.fold_in(key, 23)
    counts = jax.random.randint(first, (DEVICES,), max(1, 3 * TILES_DEV // 4), TILES_DEV + 1)
    filled = jax.random.randint(second, (), 0, DEVICES)
    return counts.at[filled].set(TILES_DEV).astype(jnp.int32)


def place_ends(entries, stream_key, least, high):
    longest = entries.shape.index(max(entries.shape))
    spots = []
    for shift in (0, 1):
        where = [jax.random.randint(jax.random.fold_in(stream_key, axis), (), 0, length) for axis, length in enumerate(entries.shape)]
        where[longest] = (where[longest] + shift) % entries.shape[longest]
        spots.append(tuple(where))
    return entries.at[spots[0]].set(least).at[spots[1]].set(high)


def level_of(rng, shape, cuts, low, top_value):
    factor_of = 1.0
    for dim, blocks in cuts:
        draws = jax.random.uniform(jax.random.fold_in(jax.random.fold_in(rng, 6), dim), (blocks,), jnp.float32, low / len(cuts), top_value / len(cuts))
        factor_of = factor_of * jnp.repeat(jnp.exp(draws), shape[dim] // blocks).reshape((-1,) + (1,) * (len(shape) - 1 - dim))
    return factor_of


def deal_out(key, own, number, rows, count, top, reach, slope):
    sequence = jax.random.permutation(key, count)
    crowded, usual = shares(count, rows * top, reach, slope, True), shares(count, rows * top, reach, slope, False)
    places = jnp.arange(count)

    def named(tallies, turn):
        used = int((tallies > 0).sum())
        fixed = max(1, used // 4)
        shifted = fixed + (places - fixed + turn * (used - fixed)) % max(1, count - fixed)
        return jnp.zeros((count,), jnp.int32).at[sequence[jnp.where(places < fixed, places, shifted)]].set(jnp.asarray(tallies, jnp.int32))

    tallies = jnp.where(number % 4 == 0, named(crowded, number // 4), named(usual, number - number // 4 - 1))
    mixed = jax.random.permutation(jax.random.fold_in(own, 3), count)
    donor, sink = mixed[0:count // 2 * 2:2], mixed[1:count // 2 * 2:2]
    room = jnp.minimum(tallies[donor] - 1, reach - tallies[sink]) // 2
    room = jnp.where((donor == sequence[0]) | (sink == sequence[0]) | (tallies[sink] == 0), 0, jnp.maximum(room, 0))
    shifted = jax.random.randint(jax.random.fold_in(own, 4), (count // 2,), 0, 1 << 20) % (room + 1)
    tallies = tallies.at[donor].add(-shifted).at[sink].add(shifted)
    labels = jnp.searchsorted(jnp.cumsum(tallies), jnp.arange(rows * top), side="right").astype(jnp.int32)
    grid = labels.reshape(top, rows).T
    grid = grid[jax.random.permutation(jax.random.fold_in(own, 1), rows)]
    turn = jax.random.randint(jax.random.fold_in(own, 2), (rows, 1), 0, top)
    return jnp.take_along_axis(grid, (jnp.arange(top)[None, :] + turn) % top, axis=1)


def shares(amount, total, bound, skew, full):
    weights = [(1 << 20) // math.isqrt(standing ** skew) + 1 for standing in range(1, amount + 1)]
    largest = bound if full else min(bound, max(-(-total // amount), total * weights[0] // sum(weights)))
    least = 1 if total - largest >= amount - 1 else 0
    given, spare = [largest] + [least] * (amount - 1), total - largest - least * (amount - 1)
    while spare > 0:
        movable = [i for i in range(1, amount) if given[i] < largest] or [i for i in range(1, amount) if given[i] < bound]
        whole, budget = sum([weights[i] for i in movable]), spare
        for i in movable:
            more = min(bound - given[i], max(1, budget * weights[i] // whole), spare)
            given[i] = given[i] + more
            spare = spare - more
    return np.array(given)


def bell_draw(rng, shape, scale, most, cuts=(), kind=jnp.bfloat16):
    result = jax.random.normal(rng, shape, jnp.float32) * scale
    if len(cuts) > 0:
        result = level_of(rng, shape, cuts, -0.22, 0.18) * result
    return jnp.clip(result, min=-most, max=most).astype(kind)


def setup_inputs(seed: int = 0) -> dict:
    arg_keys = jax.random.split(jax.random.key(seed), 7)
    brick_ids_keys = jax.random.split(jax.random.fold_in(arg_keys[0], 1), TILES // TILES_DEV)
    brick_ids_turns = jax.random.permutation(jax.random.fold_in(arg_keys[0], 3), TILES // TILES_DEV)
    brick_ids = jax.vmap(lambda own, number: deal_out(jax.random.fold_in(arg_keys[0], 2), own, number, TILES_DEV, DEVICES, 1, CAP, 2))(brick_ids_keys, brick_ids_turns).reshape((TILES, 1))
    voxel_offset = place_ends(jax.random.randint(arg_keys[1], (TILES, TILE), 0, BX * BY * BZ), jax.random.fold_in(arg_keys[1], 1), 0, (BX * BY * BZ) - 1).astype(jnp.int32)
    fractions = jnp.clip(1.0 * jax.random.uniform(arg_keys[2], (TILES, 3, TILE), jnp.float32) ** level_of(arg_keys[2], (TILES, 3, TILE), ((0, 32),), -0.2, 0.2), 0.0, 1.0)
    normals = bell_draw(arg_keys[3], (TILES, 3, TILE), 1.0, 6.0, ((0, 32),), jnp.float32)
    point_weight = jnp.clip(jnp.exp(math.log(10.0) - 4.6051702 * jax.random.uniform(arg_keys[4], (TILES, TILE), jnp.float32) ** level_of(arg_keys[4], (TILES, TILE), ((0, 32),), -0.2, 0.2)), 0.1, 10.0)
    tile_count = draw_tile_count(jax.random.fold_in(arg_keys[6], 71), 0)
    return dict(brick_ids=brick_ids, voxel_offset=voxel_offset, fractions=fractions, normals=normals, point_weight=point_weight, tile_count=tile_count)


def spline(frac):
    weights = jnp.stack([0.5 * (1.0 - frac) ** 2, 0.75 - (frac - 0.5) ** 2, 0.5 * frac * frac])
    slopes = jnp.stack([frac - 1.0, 1.0 - 2.0 * frac, frac])
    return weights, slopes


def rounded(value):
    return value.astype(jnp.bfloat16).astype(jnp.float32)


def reference(brick_ids, voxel_offset, fractions, normals, point_weight, tile_count):
    pad_y = NY + 2
    pad_z = NZ + 2
    total = (NX + 2) * pad_y * pad_z
    dest_all = brick_ids[:, 0].reshape(DEVICES, TILES_DEV)
    off_all = voxel_offset.reshape(DEVICES, TILES_DEV, TILE)
    frac_all = fractions.reshape(DEVICES, TILES_DEV, 3, TILE)
    norm_all = normals.reshape(DEVICES, TILES_DEV, 3, TILE)
    weight_all = point_weight.reshape(DEVICES, TILES_DEV, TILE)
    stencil = jnp.arange(3, dtype=jnp.int32)

    def step(carry, items):
        rhs_flat, screen_flat = carry
        dest, offset, frac, normal, weight, count = items
        valid = (jnp.arange(TILES_DEV, dtype=jnp.int32) < count).astype(jnp.float32)[:, None]
        normal = normal * valid[:, None, :]
        weight = weight * valid
        cell_x = offset // (BY * BZ)
        cell_y = (offset // BZ) % BY
        cell_z = offset % BZ
        base_x = (dest // N_YZ)[:, None] * BX + cell_x
        base_y = (dest % N_YZ)[:, None] * BY + cell_y
        wx, gx = spline(frac[:, 0])
        wy, gy = spline(frac[:, 1])
        wz, gz = spline(frac[:, 2])
        nx = normal[:, 0]
        ny = normal[:, 1]
        nz = normal[:, 2]
        a12 = rounded(nx[None, None] * gx[:, None] * wy[None, :] + ny[None, None] * wx[:, None] * gy[None, :])
        a3 = rounded(nz[None, None] * wx[:, None] * wy[None, :])
        a_s = rounded(weight[None, None] * wx[:, None] * wy[None, :])
        zb = rounded(wz)
        zd = rounded(gz)
        rhs_terms = a12[:, :, None] * zb[None, None] + a3[:, :, None] * zd[None, None]
        screen_terms = a_s[:, :, None] * zb[None, None]
        index = ((base_x[None, None, None] + stencil[:, None, None, None, None]) * pad_y
                 + base_y[None, None, None] + stencil[None, :, None, None, None]) * pad_z \
            + cell_z[None, None, None] + stencil[None, None, :, None, None]
        index = index.astype(jnp.int32).ravel()
        rhs_flat = rhs_flat.at[index].add(rhs_terms.ravel())
        screen_flat = screen_flat.at[index].add(screen_terms.ravel())
        return (rhs_flat, screen_flat), None

    start = (jnp.zeros((total,), jnp.float32), jnp.zeros((total,), jnp.float32))
    (rhs_flat, screen_flat), _ = lax.scan(step, start, (dest_all, off_all, frac_all, norm_all, weight_all, tile_count))
    rhs = rhs_flat.reshape(NX + 2, pad_y, pad_z)[1:-1, 1:-1, 1:-1]
    screen = screen_flat.reshape(NX + 2, pad_y, pad_z)[1:-1, 1:-1, 1:-1]
    return (rhs, screen)
```

```python
import functools

import jax
import jax.numpy as jnp
from jax import lax
from jax.experimental import pallas as pl
from jax.experimental.pallas import tpu as pltpu
from jax.sharding import PartitionSpec as P

BX = 4
BY = 8
BZ = 128
MESH = pl.DeviceIdType.MESH
F32, BF16, I32 = jnp.float32, jnp.bfloat16, jnp.int32
LANES = 128
SUB = 8
HALO_X = BX + 2
HALO_Y = BY + 2
ROWS = HALO_Y * SUB
CHUNKS = 2
GROUP = 4
CX, WX, GX, NRM, WGT, YW, YG, WZ, GZ = 0, 1, 4, 7, 10, 11, 11 + HALO_Y, 11 + 2 * HALO_Y, 14 + 2 * HALO_Y
CHANNELS = 17 + 2 * HALO_Y


def spline(frac):
    weights = [0.5 * (1.0 - frac) ** 2, 0.75 - (frac - 0.5) ** 2, 0.5 * frac * frac]
    slopes = [frac - 1.0, 1.0 - 2.0 * frac, frac]
    return (weights, slopes)


def pick(masks, values):
    out = jnp.zeros_like(values[0])
    for mask, value in zip(masks, values):
        out = jnp.where(mask, value, out)
    return out


def twice(value):
    return jnp.concatenate([value, value], axis=0).astype(BF16)


def pair_up(upper, lower):
    return jnp.concatenate([upper, lower], axis=0).astype(BF16)


def prepare(rows, off_ref, frac_ref, norm_ref, weight_ref, chan, cell_z):
    z_bits, y_bits = BZ.bit_length() - 1, BY.bit_length() - 1
    for half in range(chan.shape[0]):
        cols = pl.ds(half * LANES, LANES)

        def keep(n, value):
            chan[half, n, rows, :] = value

        offset = off_ref[rows, cols]
        keep(CX, (offset >> (z_bits + y_bits)).astype(F32))
        cell_z[half, rows, :] = offset & (BZ - 1)
        cell_y = (offset >> z_bits) & (BY - 1)
        wx, gx = spline(frac_ref[0, rows, cols])
        wy, gy = spline(frac_ref[1, rows, cols])
        wz, gz = spline(frac_ref[2, rows, cols])
        for k in range(3):
            keep(WX + k, wx[k])
            keep(GX + k, gx[k])
            keep(NRM + k, norm_ref[k, rows, cols])
            keep(WZ + k, wz[k])
            keep(GZ + k, gz[k])
        keep(WGT, weight_ref[rows, cols])
        at = [cell_y == m for m in range(BY)]
        for y in range(HALO_Y):
            taps = [k for k in range(3) if 0 <= y - k < BY]
            keep(YW + y, pick([at[y - k] for k in taps], [wy[k] for k in taps]))
            keep(YG + y, pick([at[y - k] for k in taps], [gy[k] for k in taps]))


def brick_table(capacity, slots, dest, count):
    tiles = dest.shape[1]
    across = jnp.broadcast_to(dest, (tiles, tiles))
    down = jnp.transpose(across)
    later = lax.broadcasted_iota(I32, (tiles, tiles), 0)
    sooner = lax.broadcasted_iota(I32, (tiles, tiles), 1)
    earlier = (across == down) & (sooner < later) & (sooner < count)
    rank = jnp.sum(jnp.where(earlier, 1, 0), axis=1, keepdims=True)
    tile = lax.broadcasted_iota(I32, (tiles, 1), 0)
    slot = jnp.where(tile < count, down[:, :1] * capacity + rank, -1)
    wanted = lax.broadcasted_iota(I32, (tiles, slots), 1)
    found = jnp.where(slot == wanted, jnp.broadcast_to(tile, (tiles, slots)), -1)
    return jnp.max(found, axis=0, keepdims=True)


def fused_kernel(
    capacity, n_slabs, n_columns, dest_hbm, count_hbm, off_hbm, frac_hbm, norm_hbm, weight_hbm, rhs_ref, screen_ref,
    dest, off, frac, norm, weight, table_v, table, chan, cell_z, grid,
    parts, core_in, mine, peer_in, ready, main_in, low_in, tail_low, tail_high,
    load_sem, core_sem, peer_sem, main_sem, low_sem, tail_sem,
):
    tiles, tile_len = off.shape
    halves = tile_len // LANES
    n_chips = n_columns // 2
    last = n_slabs - 1
    me_x, me_y = lax.axis_index("gx"), lax.axis_index("yz")
    me_c, me_b = me_y // 2, lax.rem(me_y, 2)

    def slab_of(step):
        return lax.rem(me_x + 1 + step, n_slabs)

    def slab_at(hop):
        return lax.rem(me_x + hop + n_slabs, n_slabs)

    def column_at(hop):
        return 2 * lax.rem(me_c + hop, n_chips) + me_b

    loads = [
        pltpu.make_async_copy(dest_hbm, dest, load_sem.at[0]),
    ]
    span = tiles // CHUNKS
    chunks = []
    for n in range(CHUNKS):
        rows = pl.ds(n * span, span)
        base = 3 + 4 * n
        chunks.append([
            pltpu.make_async_copy(off_hbm.at[rows], off.at[rows], load_sem.at[base]),
            pltpu.make_async_copy(frac_hbm.at[:, rows], frac.at[:, rows], load_sem.at[base + 1]),
            pltpu.make_async_copy(norm_hbm.at[:, rows], norm.at[:, rows], load_sem.at[base + 2]),
            pltpu.make_async_copy(weight_hbm.at[rows], weight.at[rows], load_sem.at[base + 3]),
        ])
    for copy in loads + sum(chunks, []):
        copy.start()

    barrier = pltpu.get_barrier_semaphore()
    friends = [(me_x, me_y + 1 - 2 * me_b)]
    friends += [(slab_at(z), column_at(c)) for z in range(n_slabs) for c in range(n_chips) if z or c]
    for friend in friends:
        pl.semaphore_signal(barrier, inc=1, device_id=friend, device_id_type=MESH)

    grid[...] = jnp.zeros_like(grid)

    for copy in loads:
        copy.wait()
    table_v[...] = brick_table(capacity, table_v.shape[1], dest[...], count_hbm[0])

    def prepare_rows(step, _):
        prepare(pl.ds(pl.multiple_of(step * SUB, SUB), SUB), off, frac, norm, weight, chan, cell_z)
        return 0

    table_copy = pltpu.make_async_copy(table_v, table, load_sem.at[2])
    for n in range(CHUNKS):
        for copy in chunks[n]:
            copy.wait()
        if n == CHUNKS - 1:
            table_copy.start()
        lax.fori_loop(n * span // SUB, (n + 1) * span // SUB, prepare_rows, 0)
    table_copy.wait()

    sub = lax.broadcasted_iota(I32, (SUB, LANES), 0)

    def layer_of(slab):
        return (sub + 4 * lax.rem(slab, 2)) & (SUB - 1)

    def brick_sum(g):
        slab = slab_of(g // n_columns)
        brick = slab * n_columns + lax.rem(g, n_columns)
        layer = layer_of(slab)
        outside = ((layer == 0) & (slab == 0)) | ((layer == HALO_X - 1) & (slab == last))
        layer = jnp.where(outside, -SUB, layer).astype(F32)
        out = None
        for c in range(capacity):
            lefts, rights = [], []
            entry = table[0, brick * capacity + c]
            away = jnp.where(entry >= 0, 0.0, 8.0 * SUB)
            tile = jnp.minimum(jnp.maximum(entry, 0), tiles - 1)
            for half in range(halves):
                left, right = [[], [], []], [[], []]

                def row(n):
                    return jnp.broadcast_to(chan[half, n, pl.ds(tile, 1), :], (SUB, LANES))

                gap = layer - (row(CX) + away)
                hit = [gap == float(k) for k in range(3)]
                wx = pick(hit, [row(WX + k) for k in range(3)])
                gx = pick(hit, [row(GX + k) for k in range(3)])
                first, second = gx * row(NRM), wx * row(NRM + 1)
                third, plain = twice(wx * row(NRM + 2)), twice(wx * row(WGT))
                for m in range(HALO_Y // 2):
                    wy = [row(YW + 2 * m), row(YW + 2 * m + 1)]
                    gy = [row(YG + 2 * m), row(YG + 2 * m + 1)]
                    both = pair_up(first * wy[0] + second * gy[0], first * wy[1] + second * gy[1])
                    wide = pair_up(wy[0], wy[1])
                    left[0].append(both)
                    left[1].append(plain * wide)
                    left[2].append(third * wide)
                z = jnp.broadcast_to(cell_z[half, pl.ds(tile, 1), :], (SUB, LANES))
                tap = (sub - z + 1) & (SUB - 1)
                hit = [tap == k for k in range(3)]
                value = twice(pick(hit, [row(WZ + k) for k in range(3)]))
                slope = twice(pick(hit, [row(GZ + k) for k in range(3)]))
                home = ((z - 1 + tap) >> 3).astype(F32)
                home = pair_up(home, home - 1.0)
                zero = jnp.zeros_like(value)
                for m in range(BZ // (2 * SUB)):
                    here = home == jnp.bfloat16(2 * m)
                    right[0].append(jnp.where(here, value, zero))
                    right[1].append(jnp.where(here, slope, zero))
                lefts.append(jnp.concatenate(sum(left, []), axis=0))
                rights.append(jnp.concatenate(sum(right, []), axis=0))
            dims = (((1,), (1,)), ((), ()))
            more = lax.dot_general(
                jnp.concatenate(lefts, axis=1), jnp.concatenate(rights, axis=1), dims, preferred_element_type=F32
            )
            out = more if out is None else out + more
        return out

    def add_brick(g):
        out = brick_sum(g)
        rhs = out[:ROWS, :BZ] + out[2 * ROWS :, BZ:]
        screen = out[ROWS : 2 * ROWS, :BZ]
        step, column = g // n_columns, lax.rem(g, n_columns)
        carried = (layer_of(slab_of(step)) < 2) & (step > 0)
        edge = carried | (column > 0)
        for f, field in enumerate((rhs, screen)):
            for y in range(HALO_Y):
                at = pl.ds(pl.multiple_of((column * BY + y) * SUB, SUB), SUB)
                old = jnp.where(edge if y < 2 else carried, grid[f, at, :], 0.0)
                grid[f, at, :] = field[y * SUB : (y + 1) * SUB] + old

    def core_copy(j):
        layers = pl.ds(0, HALO_X if j == last else BX)
        return pltpu.make_async_remote_copy(
            src_ref=parts.at[j, 1 - me_b, :, layers],
            dst_ref=core_in.at[j, :, layers],
            send_sem=core_sem.at[0, j],
            recv_sem=core_sem.at[1, j],
            device_id=(me_x, me_y + 1 - 2 * me_b),
            device_id_type=MESH,
        )

    def peer_copy(j, hop):
        return pltpu.make_async_remote_copy(
            src_ref=mine.at[j, lax.rem(me_c + hop, n_chips), pl.ds(1 if j == last else 0, BX)],
            dst_ref=peer_in.at[j, hop],
            send_sem=peer_sem.at[0, j, hop],
            recv_sem=peer_sem.at[1, j, hop],
            device_id=(me_x, column_at(hop)),
            device_id_type=MESH,
        )

    def main_copy(j):
        return pltpu.make_async_remote_copy(
            src_ref=ready.at[j, pl.ds(1, BX - 1)],
            dst_ref=main_in.at[j],
            send_sem=main_sem.at[0, j],
            recv_sem=main_sem.at[1, j],
            device_id=(slab_at(1 + j), me_y),
            device_id_type=MESH,
        )

    def low_copy(j):
        return pltpu.make_async_remote_copy(
            src_ref=ready.at[j, 0],
            dst_ref=low_in.at[j],
            send_sem=low_sem.at[0, j],
            recv_sem=low_sem.at[1, j],
            device_id=(slab_at(j), me_y),
            device_id_type=MESH,
        )

    def tail_copy(side, hop):
        layer, target, to = ((0, tail_low, -1), (HALO_X - 1, tail_high, 1))[side]
        return pltpu.make_async_remote_copy(
            src_ref=mine.at[last, lax.rem(me_c + hop, n_chips), layer],
            dst_ref=target.at[hop],
            send_sem=tail_sem.at[0, side, hop],
            recv_sem=tail_sem.at[1, side, hop],
            device_id=(slab_at(to), column_at(hop)),
            device_id_type=MESH,
        )

    def share(j):
        start = 4 * lax.rem(slab_of(j), 2)
        for layer in range(HALO_X if j == last else BX):
            at = lax.rem(start + layer, SUB)
            for column in range(n_columns):
                for f in range(2):
                    rows = pl.ds((column * BY + 1) * SUB + at, BY, stride=SUB)
                    parts[j, column % 2, column // 2, layer, f] = grid[f, rows, :]
        core_copy(j).start()

    def spread(j):
        core_copy(j).wait()
        for chip in range(n_chips):
            for layer in range(HALO_X if j == last else BX):
                mine[j, chip, layer] = parts[j, me_b, chip, layer] + core_in[j, chip, layer]
        for hop in range(1, n_chips):
            peer_copy(j, hop).start()
        if j == last:
            for hop in range(n_chips):
                tail_copy(0, hop).start()

            @pl.when(me_x < last)
            def _():
                for hop in range(n_chips):
                    tail_copy(1, hop).start()

    def forward(j):
        for hop in range(1, n_chips):
            peer_copy(j, hop).wait()
        for layer in range(BX):
            total = mine[j, me_c, layer]
            for hop in range(1, n_chips):
                total = total + peer_in[j, hop, layer]
            ready[j, layer] = total
        main_copy(j).start()
        if j > 0:
            low_copy(j).start()

    group = min(GROUP, n_columns)
    turns = n_columns // group
    pl.semaphore_wait(barrier, len(friends))
    for step in range(n_slabs):

        def turn(p, _):
            for k in range(group):
                add_brick(step * n_columns + p * group + k)
            if step > 0:
                @pl.when(p == max(0, turns - 2))
                def _():
                    spread(step - 1)

            return 0

        lax.fori_loop(0, turns, turn, 0)
        share(step)
    early = n_slabs - 2
    for j in range(0, max(0, early - 1)):
        forward(j)
    spread(last)
    for j in range(max(0, early - 1), last):
        forward(j)

    outs = (rhs_ref, screen_ref)
    for j in range(last):
        main_copy(j).wait()
        if j > 0:
            low_copy(j).wait()
    for hop in range(1, n_chips):
        peer_copy(last, hop).wait()
    for hop in range(n_chips):
        tail_copy(0, hop).wait()
    for layer in range(BX):
        total = mine[last, me_c, layer + 1]
        for hop in range(1, n_chips):
            total = total + peer_in[last, hop, layer]
        if layer < BX - 1:
            for j in range(last):
                total = total + main_in[j, layer]
        else:
            total = total + ready[0, 0]
            for j in range(1, last):
                total = total + low_in[j]
            for hop in range(n_chips):
                total = total + tail_low[hop]
        for f in range(2):
            outs[f][layer] = total[f]

    @pl.when(me_x < last)
    def _():
        for hop in range(n_chips):
            tail_copy(1, hop).wait_send()

    @pl.when(me_x > 0)
    def _():
        for hop in range(n_chips):
            tail_copy(1, hop).wait_recv()
        for f in range(2):
            total = outs[f][0]
            for hop in range(n_chips):
                total = total + tail_high[hop, f]
            outs[f][0] = total


def fused(capacity, n_slabs, n_columns, dest, count, off, frac, norm, weight):
    tiles, tile_len = off.shape
    slots = n_slabs * n_columns * capacity
    n_chips = n_columns // 2
    block = (2, BY, BZ)
    dma = pltpu.SemaphoreType.DMA
    out = jax.ShapeDtypeStruct((BX, BY, BZ), F32)
    return pl.pallas_call(
        functools.partial(fused_kernel, capacity, n_slabs, n_columns),
        out_shape=(out, out),
        in_specs=[pl.BlockSpec(memory_space=pltpu.HBM), pl.BlockSpec(memory_space=pltpu.SMEM)] + [pl.BlockSpec(memory_space=pltpu.HBM)] * 4,
        out_specs=(pl.BlockSpec(memory_space=pltpu.VMEM),) * 2,
        scratch_shapes=[
            pltpu.VMEM((1, tiles), I32),
            pltpu.VMEM((tiles, tile_len), I32),
            pltpu.VMEM((3, tiles, tile_len), F32),
            pltpu.VMEM((3, tiles, tile_len), F32),
            pltpu.VMEM((tiles, tile_len), F32),
            pltpu.VMEM((1, slots), I32),
            pltpu.SMEM((1, slots), I32),
            pltpu.VMEM((tile_len // LANES, CHANNELS, tiles + SUB, LANES), F32),
            pltpu.VMEM((tile_len // LANES, tiles, LANES), I32),
            pltpu.VMEM((2, (n_columns * BY + 2) * SUB, BZ), F32),
            pltpu.VMEM((n_slabs, 2, n_chips, HALO_X) + block, F32),
            pltpu.VMEM((n_slabs, n_chips, HALO_X) + block, F32),
            pltpu.VMEM((n_slabs, n_chips, HALO_X) + block, F32),
            pltpu.VMEM((n_slabs, n_chips, BX) + block, F32),
            pltpu.VMEM((n_slabs, BX) + block, F32),
            pltpu.VMEM((n_slabs, BX - 1) + block, F32),
            pltpu.VMEM((n_slabs,) + block, F32),
            pltpu.VMEM((n_chips,) + block, F32),
            pltpu.VMEM((n_chips,) + block, F32),
            dma((3 + 4 * CHUNKS,)),
            dma((2, n_slabs)),
            dma((2, n_slabs, n_chips)),
            dma((2, n_slabs)),
            dma((2, n_slabs)),
            dma((2, 2, n_chips)),
        ],
        compiler_params=pltpu.CompilerParams(collective_id=0, has_side_effects=True),
        name="fused",
    )(dest, count, off, frac, norm, weight)


def shards(brick_ids, voxel_offset, fractions, normals, point_weight, tile_count):
    n_slabs = lax.axis_size("gx")
    n_columns = lax.axis_size("yz")
    devices = n_slabs * n_columns
    tiles_here = brick_ids.shape[0]
    capacity = max(2, (tiles_here + devices - 1) // devices)
    return fused(
        capacity, n_slabs, n_columns, brick_ids.reshape(1, tiles_here), tile_count, voxel_offset,
        jnp.transpose(fractions, (1, 0, 2)), jnp.transpose(normals, (1, 0, 2)), point_weight,
    )


def solution(mesh):
    return jax.shard_map(
        shards,
        mesh=mesh,
        in_specs=(
            P(("gx", "yz"), None),
            P(("gx", "yz"), None),
            P(("gx", "yz"), None, None),
            P(("gx", "yz"), None, None),
            P(("gx", "yz"), None),
            P(("gx", "yz")),
        ),
        out_specs=(P("gx", "yz", None), P("gx", "yz", None)),
        check_vma=False,
    )
```

```python
import functools

import jax
import jax.numpy as jnp
from jax import lax
from jax.experimental import pallas as pl
from jax.experimental.pallas import tpu as pltpu
from jax.sharding import PartitionSpec as P

BX = 4
BY = 8
BZ = 128
MESH = pl.DeviceIdType.MESH
F32, BF16, I32 = jnp.float32, jnp.bfloat16, jnp.int32
LANES = 128
SUB = 8
HALO_X = BX + 2
HALO_Y = BY + 2
ROWS = HALO_Y * SUB
CHUNKS = 2
CX, WX, GX, NRM, WGT, YW, YG, WZ, GZ = 0, 1, 4, 7, 10, 11, 11 + HALO_Y, 11 + 2 * HALO_Y, 14 + 2 * HALO_Y
CHANNELS = 17 + 2 * HALO_Y


def spline(frac):
    weights = [0.5 * (1.0 - frac) ** 2, 0.75 - (frac - 0.5) ** 2, 0.5 * frac * frac]
    slopes = [frac - 1.0, 1.0 - 2.0 * frac, frac]
    return (weights, slopes)


def pick(masks, values):
    out = jnp.zeros_like(values[0])
    for mask, value in zip(masks, values):
        out = jnp.where(mask, value, out)
    return out


def twice(value):
    return jnp.concatenate([value, value], axis=0).astype(BF16)


def pair_up(upper, lower):
    return jnp.concatenate([upper, lower], axis=0).astype(BF16)


def prepare(rows, off_ref, frac_ref, norm_ref, weight_ref, chan, cell_z):
    z_bits, y_bits = BZ.bit_length() - 1, BY.bit_length() - 1
    for half in range(chan.shape[0]):
        cols = pl.ds(half * LANES, LANES)

        def keep(n, value):
            chan[half, n, rows, :] = value

        offset = off_ref[rows, cols]
        keep(CX, (offset >> (z_bits + y_bits)).astype(F32))
        cell_z[half, rows, :] = offset & (BZ - 1)
        cell_y = (offset >> z_bits) & (BY - 1)
        wx, gx = spline(frac_ref[0, rows, cols])
        wy, gy = spline(frac_ref[1, rows, cols])
        wz, gz = spline(frac_ref[2, rows, cols])
        for k in range(3):
            keep(WX + k, wx[k])
            keep(GX + k, gx[k])
            keep(NRM + k, norm_ref[k, rows, cols])
            keep(WZ + k, wz[k])
            keep(GZ + k, gz[k])
        keep(WGT, weight_ref[rows, cols])
        at = [cell_y == m for m in range(BY)]
        for y in range(HALO_Y):
            taps = [k for k in range(3) if 0 <= y - k < BY]
            keep(YW + y, pick([at[y - k] for k in taps], [wy[k] for k in taps]))
            keep(YG + y, pick([at[y - k] for k in taps], [gy[k] for k in taps]))


def brick_table(capacity, slots, dest, count):
    tiles = dest.shape[1]
    across = jnp.broadcast_to(dest, (tiles, tiles))
    down = jnp.transpose(across)
    later = lax.broadcasted_iota(I32, (tiles, tiles), 0)
    sooner = lax.broadcasted_iota(I32, (tiles, tiles), 1)
    earlier = (across == down) & (sooner < later) & (sooner < count)
    rank = jnp.sum(jnp.where(earlier, 1, 0), axis=1, keepdims=True)
    tile = lax.broadcasted_iota(I32, (tiles, 1), 0)
    slot = jnp.where(tile < count, down[:, :1] * capacity + rank, -1)
    wanted = lax.broadcasted_iota(I32, (tiles, slots), 1)
    found = jnp.where(slot == wanted, jnp.broadcast_to(tile, (tiles, slots)), -1)
    return jnp.max(found, axis=0, keepdims=True)


def fused_kernel(
    capacity, n_slabs, n_columns, dest_hbm, count_hbm, off_hbm, frac_hbm, norm_hbm, weight_hbm, out_ref,
    dest, off, frac, norm, weight, table_v, table, chan, cell_z, grid,
    parts, core_in, mine, peer_in, ready, main_in, low_in, tail_low, tail_high,
    load_sem, core_sem, peer_sem, main_sem, low_sem, tail_sem,
):
    tiles, tile_len = off.shape
    halves = tile_len // LANES
    n_chips = n_columns // 2
    near = n_chips // 2
    last = n_slabs - 1
    me_x, me_y = lax.axis_index("gx"), lax.axis_index("yz")
    me_c, me_b = me_y // 2, lax.rem(me_y, 2)
    me_h, me_r = me_c // near, lax.rem(me_c, near)
    first_column = (n_columns // 2 - 1) * (1 - me_h)

    def slab_of(step):
        return lax.rem(me_x + 1 + step, n_slabs)

    def slab_at(hop):
        return lax.rem(me_x + hop + n_slabs, n_slabs)

    def column_at(hop):
        return 2 * lax.rem(me_c + hop, n_chips) + me_b

    def half_at(part):
        return lax.rem(me_h + 1 + part, 2)

    def place(part, turn):
        return lax.rem(me_r + turn, near)

    def hop_to(part, turn):
        return lax.rem(half_at(part) * near + place(part, turn) - me_c + n_chips, n_chips)

    loads = [
        pltpu.make_async_copy(dest_hbm, dest, load_sem.at[0]),
    ]
    span = tiles // CHUNKS
    chunks = []
    for n in range(CHUNKS):
        rows = pl.ds(n * span, span)
        base = 3 + 4 * n
        chunks.append([
            pltpu.make_async_copy(off_hbm.at[rows], off.at[rows], load_sem.at[base]),
            pltpu.make_async_copy(frac_hbm.at[:, rows], frac.at[:, rows], load_sem.at[base + 1]),
            pltpu.make_async_copy(norm_hbm.at[:, rows], norm.at[:, rows], load_sem.at[base + 2]),
            pltpu.make_async_copy(weight_hbm.at[rows], weight.at[rows], load_sem.at[base + 3]),
        ])
    for copy in loads + sum(chunks, []):
        copy.start()

    barrier = pltpu.get_barrier_semaphore()
    friends = [(me_x, me_y + 1 - 2 * me_b)]
    friends += [(slab_at(z), column_at(c)) for z in range(n_slabs) for c in range(n_chips) if z or c]
    for friend in friends:
        pl.semaphore_signal(barrier, inc=1, device_id=friend, device_id_type=MESH)

    grid[...] = jnp.zeros_like(grid)

    for copy in loads:
        copy.wait()
    table_v[...] = brick_table(capacity, table_v.shape[1], dest[...], count_hbm[0])

    def prepare_rows(step, _):
        prepare(pl.ds(pl.multiple_of(step * SUB, SUB), SUB), off, frac, norm, weight, chan, cell_z)
        return 0

    table_copy = pltpu.make_async_copy(table_v, table, load_sem.at[2])
    for n in range(CHUNKS):
        for copy in chunks[n]:
            copy.wait()
        if n == CHUNKS - 1:
            table_copy.start()
        lax.fori_loop(n * span // SUB, (n + 1) * span // SUB, prepare_rows, 0)
    table_copy.wait()

    sub = lax.broadcasted_iota(I32, (SUB, LANES), 0)

    def layer_of(slab):
        return (sub + 4 * lax.rem(slab, 2)) & (SUB - 1)

    def brick_sum(step, column):
        slab = slab_of(step)
        brick = slab * n_columns + column
        layer = layer_of(slab)
        outside = ((layer == 0) & (slab == 0)) | ((layer == HALO_X - 1) & (slab == last))
        layer = jnp.where(outside, -SUB, layer).astype(F32)
        out = None
        for c in range(capacity):
            lefts, rights = [], []
            entry = table[0, brick * capacity + c]
            away = jnp.where(entry >= 0, 0.0, 8.0 * SUB)
            tile = jnp.minimum(jnp.maximum(entry, 0), tiles - 1)
            for half in range(halves):
                left, right = [[], [], []], [[], []]

                def row(n):
                    return jnp.broadcast_to(chan[half, n, pl.ds(tile, 1), :], (SUB, LANES))

                gap = layer - (row(CX) + away)
                hit = [gap == float(k) for k in range(3)]
                wx = pick(hit, [row(WX + k) for k in range(3)])
                gx = pick(hit, [row(GX + k) for k in range(3)])
                first, second = gx * row(NRM), wx * row(NRM + 1)
                third, plain = twice(wx * row(NRM + 2)), twice(wx * row(WGT))
                for m in range(HALO_Y // 2):
                    wy = [row(YW + 2 * m), row(YW + 2 * m + 1)]
                    gy = [row(YG + 2 * m), row(YG + 2 * m + 1)]
                    both = pair_up(first * wy[0] + second * gy[0], first * wy[1] + second * gy[1])
                    wide = pair_up(wy[0], wy[1])
                    left[0].append(both)
                    left[1].append(plain * wide)
                    left[2].append(third * wide)
                z = jnp.broadcast_to(cell_z[half, pl.ds(tile, 1), :], (SUB, LANES))
                tap = (sub - z + 1) & (SUB - 1)
                hit = [tap == k for k in range(3)]
                value = twice(pick(hit, [row(WZ + k) for k in range(3)]))
                slope = twice(pick(hit, [row(GZ + k) for k in range(3)]))
                home = ((z - 1 + tap) >> 3).astype(F32)
                home = pair_up(home, home - 1.0)
                zero = jnp.zeros_like(value)
                for m in range(BZ // (2 * SUB)):
                    here = home == jnp.bfloat16(2 * m)
                    right[0].append(jnp.where(here, value, zero))
                    right[1].append(jnp.where(here, slope, zero))
                lefts.append(jnp.concatenate(sum(left, []), axis=0))
                rights.append(jnp.concatenate(sum(right, []), axis=0))
            dims = (((1,), (1,)), ((), ()))
            more = lax.dot_general(
                jnp.concatenate(lefts, axis=1), jnp.concatenate(rights, axis=1), dims, preferred_element_type=F32
            )
            out = more if out is None else out + more
        return out

    def add_brick(step, k):
        column = lax.rem(first_column + k, n_columns)
        out = brick_sum(step, column)
        rhs = out[:ROWS, :BZ] + out[2 * ROWS :, BZ:]
        screen = out[ROWS : 2 * ROWS, :BZ]
        carried = (layer_of(slab_of(step)) < 2) & (step > 0)
        below = carried | (column > 0) if k > 0 else carried
        above = carried | (first_column > 0) if k == n_columns - 1 else carried
        for f, field in enumerate((rhs, screen)):
            for y in range(HALO_Y):
                at = pl.ds(pl.multiple_of((column * BY + y) * SUB, SUB), SUB)
                keep = below if y < 2 else above if y >= BY else carried
                old = jnp.where(keep, grid[f, at, :], 0.0)
                grid[f, at, :] = field[y * SUB : (y + 1) * SUB] + old

    def depth(j):
        return HALO_X if isinstance(j, int) and j == last else BX

    def core_copy(j, part):
        layers = pl.ds(0, depth(j))
        return pltpu.make_async_remote_copy(
            src_ref=parts.at[j, part, 1 - me_b, :, layers],
            dst_ref=core_in.at[j, part, :, layers],
            send_sem=core_sem.at[0, j, part],
            recv_sem=core_sem.at[1, j, part],
            device_id=(me_x, me_y + 1 - 2 * me_b),
            device_id_type=MESH,
        )

    def peer_copy(j, part, turn):
        hop = hop_to(part, turn)
        return pltpu.make_async_remote_copy(
            src_ref=mine.at[j, part, place(part, turn), pl.ds(depth(j) - BX - (depth(j) > BX), BX)],
            dst_ref=peer_in.at[j, hop],
            send_sem=peer_sem.at[0, j, hop],
            recv_sem=peer_sem.at[1, j, hop],
            device_id=(me_x, column_at(hop)),
            device_id_type=MESH,
        )

    peers = [(part, turn) for part in range(2) for turn in range(near) if (part, turn) != (1, 0)]

    def main_copy(j):
        return pltpu.make_async_remote_copy(
            src_ref=ready.at[j, pl.ds(1, BX - 1)],
            dst_ref=main_in.at[j],
            send_sem=main_sem.at[0, j],
            recv_sem=main_sem.at[1, j],
            device_id=(slab_at(1 + j), me_y),
            device_id_type=MESH,
        )

    def low_copy(j):
        return pltpu.make_async_remote_copy(
            src_ref=ready.at[j, 0],
            dst_ref=low_in.at[j],
            send_sem=low_sem.at[0, j],
            recv_sem=low_sem.at[1, j],
            device_id=(slab_at(j), me_y),
            device_id_type=MESH,
        )

    def tail_copy(side, part, turn):
        layer, target, to = ((0, tail_low, -1), (HALO_X - 1, tail_high, 1))[side]
        hop = hop_to(part, turn)
        return pltpu.make_async_remote_copy(
            src_ref=mine.at[last, part, place(part, turn), layer],
            dst_ref=target.at[hop],
            send_sem=tail_sem.at[0, side, hop],
            recv_sem=tail_sem.at[1, side, hop],
            device_id=(slab_at(to), column_at(hop)),
            device_id_type=MESH,
        )

    def share(j, part):
        start = 4 * lax.rem(slab_of(j), 2)
        base = half_at(part) * (n_columns // 2)
        for layer in range(depth(j)):
            at = lax.rem(start + layer, SUB)
            for k in range(n_columns // 2):
                for f in range(2):
                    rows = pl.ds(((base + k) * BY + 1) * SUB + at, BY, stride=SUB)
                    parts[j, part, k % 2, k // 2, layer, f] = grid[f, rows, :]
        core_copy(j, part).start()

    def spread(j, part):
        core_copy(j, part).wait()
        for chip in range(near):
            for layer in range(depth(j)):
                mine[j, part, chip, layer] = parts[j, part, me_b, chip, layer] + core_in[j, part, chip, layer]
        for turn in range(part, near):
            peer_copy(j, part, turn).start()
        if depth(j) > BX:
            for turn in range(near):
                tail_copy(0, part, turn).start()

            @pl.when(me_x < last)
            def _():
                for turn in range(near):
                    tail_copy(1, part, turn).start()

    def forward(j):
        for peer in peers:
            peer_copy(j, *peer).wait()
        for layer in range(BX):
            total = mine[j, 1, me_r, layer]
            for hop in range(1, n_chips):
                total = total + peer_in[j, hop, layer]
            ready[j, layer] = total
        main_copy(j).start()
        if j > 0:
            low_copy(j).start()

    split = n_columns // 2 + 1

    def slab_step(step, first):
        for k in range(split):
            add_brick(step, k)
        if first is None:
            spread(step - 1, 1)
        else:
            first()
        share(step, 0)
        for k in range(split, n_columns):
            add_brick(step, k)
        share(step, 1)
        spread(step, 0)

    def early_step(step, _):
        def first():
            @pl.when(step == 0)
            def _():
                pl.semaphore_wait(barrier, len(friends))

            @pl.when(step > 0)
            def _():
                spread(step - 1, 1)

        slab_step(step, first)
        return 0

    lax.fori_loop(0, last, early_step, 0)
    slab_step(last, None)
    spread(last, 1)
    for j in range(last):
        forward(j)

    for j in range(last):
        main_copy(j).wait()
        if j > 0:
            low_copy(j).wait()
    for peer in peers:
        peer_copy(last, *peer).wait()
    ends = [(part, turn) for part in range(2) for turn in range(near)]
    for end in ends:
        tail_copy(0, *end).wait()
    for layer in range(BX):
        total = mine[last, 1, me_r, layer + 1]
        for hop in range(1, n_chips):
            total = total + peer_in[last, hop, layer]
        if layer < BX - 1:
            for j in range(last):
                total = total + main_in[j, layer]
        else:
            total = total + ready[0, 0]
            for j in range(1, last):
                total = total + low_in[j]
            for hop in range(n_chips):
                total = total + tail_low[hop]
        for f in range(2):
            out_ref[f, layer] = total[f]

    @pl.when(me_x < last)
    def _():
        for end in ends:
            tail_copy(1, *end).wait_send()

    @pl.when(me_x > 0)
    def _():
        for end in ends:
            tail_copy(1, *end).wait_recv()
        for f in range(2):
            total = out_ref[f, 0]
            for hop in range(n_chips):
                total = total + tail_high[hop, f]
            out_ref[f, 0] = total


def hbm(array):
    return pltpu.with_memory_space_constraint(array, pltpu.HBM)


def fused(capacity, n_slabs, n_columns, dest, count, off, frac, norm, weight):
    tiles, tile_len = off.shape
    slots = n_slabs * n_columns * capacity
    n_chips = n_columns // 2
    block = (2, BY, BZ)
    dma = pltpu.SemaphoreType.DMA
    near = n_chips // 2
    return pl.pallas_call(
        functools.partial(fused_kernel, capacity, n_slabs, n_columns),
        out_shape=jax.ShapeDtypeStruct((2, BX, BY, BZ), F32),
        in_specs=[pl.BlockSpec(memory_space=pltpu.HBM), pl.BlockSpec(memory_space=pltpu.SMEM)] + [pl.BlockSpec(memory_space=pltpu.HBM)] * 4,
        out_specs=pl.BlockSpec(memory_space=pltpu.VMEM),
        scratch_shapes=[
            pltpu.VMEM((1, tiles), I32),
            pltpu.VMEM((tiles, tile_len), I32),
            pltpu.VMEM((3, tiles, tile_len), F32),
            pltpu.VMEM((3, tiles, tile_len), F32),
            pltpu.VMEM((tiles, tile_len), F32),
            pltpu.VMEM((1, slots), I32),
            pltpu.SMEM((1, slots), I32),
            pltpu.VMEM((tile_len // LANES, CHANNELS, tiles + SUB, LANES), F32),
            pltpu.VMEM((tile_len // LANES, tiles, LANES), I32),
            pltpu.VMEM((2, (n_columns * BY + 2) * SUB, BZ), F32),
            pltpu.VMEM((n_slabs, 2, 2, near, HALO_X) + block, F32),
            pltpu.VMEM((n_slabs, 2, near, HALO_X) + block, F32),
            pltpu.VMEM((n_slabs, 2, near, HALO_X) + block, F32),
            pltpu.VMEM((n_slabs, n_chips, BX) + block, F32),
            pltpu.VMEM((n_slabs, BX) + block, F32),
            pltpu.VMEM((n_slabs, BX - 1) + block, F32),
            pltpu.VMEM((n_slabs,) + block, F32),
            pltpu.VMEM((n_chips,) + block, F32),
            pltpu.VMEM((n_chips,) + block, F32),
            dma((3 + 4 * CHUNKS,)),
            dma((2, n_slabs, 2)),
            dma((2, n_slabs, n_chips)),
            dma((2, n_slabs)),
            dma((2, n_slabs)),
            dma((2, 2, n_chips)),
        ],
        compiler_params=pltpu.CompilerParams(collective_id=0, has_side_effects=True, vmem_limit_bytes=32 << 20),
        name="fused",
    )(hbm(dest), count, hbm(off), hbm(frac), hbm(norm), hbm(weight))


def shards(brick_ids, voxel_offset, fractions, normals, point_weight, tile_count):
    n_slabs = lax.axis_size("gx")
    n_columns = lax.axis_size("yz")
    devices = n_slabs * n_columns
    tiles_here = brick_ids.shape[0]
    capacity = max(2, (tiles_here + devices - 1) // devices)
    both = fused(
        capacity, n_slabs, n_columns, brick_ids.reshape(1, tiles_here), tile_count, voxel_offset,
        jnp.transpose(fractions, (1, 0, 2)), jnp.transpose(normals, (1, 0, 2)), point_weight,
    )
    return (both[0], both[1])


def solution(mesh):
    return jax.shard_map(
        shards,
        mesh=mesh,
        in_specs=(
            P(("gx", "yz"), None),
            P(("gx", "yz"), None),
            P(("gx", "yz"), None, None),
            P(("gx", "yz"), None, None),
            P(("gx", "yz"), None),
            P(("gx", "yz")),
        ),
        out_specs=(P("gx", "yz", None), P("gx", "yz", None)),
        check_vma=False,
    )
```

```python
import functools

import jax
import jax.numpy as jnp
from jax import lax
from jax.experimental import pallas as pl
from jax.experimental.pallas import tpu as pltpu
from jax.sharding import PartitionSpec as P

BX = 4
BY = 8
BZ = 128
MESH = pl.DeviceIdType.MESH
F32, BF16, I32 = jnp.float32, jnp.bfloat16, jnp.int32
LANES = 128
SUB = 8
HALO_X = BX + 2
HALO_Y = BY + 2
ROWS = HALO_Y * SUB
CHUNKS = 2
CX, WX, GX, NRM, WGT, YW, YG, WZ, GZ = 0, 1, 4, 7, 10, 11, 11 + HALO_Y, 11 + 2 * HALO_Y, 14 + 2 * HALO_Y
CHANNELS = 17 + 2 * HALO_Y


def spline(frac):
    weights = [0.5 * (1.0 - frac) ** 2, 0.75 - (frac - 0.5) ** 2, 0.5 * frac * frac]
    slopes = [frac - 1.0, 1.0 - 2.0 * frac, frac]
    return (weights, slopes)


def pick(masks, values):
    out = jnp.zeros_like(values[0])
    for mask, value in zip(masks, values):
        out = jnp.where(mask, value, out)
    return out


def twice(value):
    return jnp.concatenate([value, value], axis=0).astype(BF16)


def pair_up(upper, lower):
    return jnp.concatenate([upper, lower], axis=0).astype(BF16)


def prepare(rows, off_ref, frac_ref, norm_ref, weight_ref, chan, cell_z):
    z_bits, y_bits = BZ.bit_length() - 1, BY.bit_length() - 1
    for half in range(chan.shape[0]):
        cols = pl.ds(half * LANES, LANES)

        def keep(n, value):
            chan[half, n, rows, :] = value

        offset = off_ref[rows, cols]
        keep(CX, (offset >> (z_bits + y_bits)).astype(F32))
        cell_z[half, rows, :] = offset & (BZ - 1)
        cell_y = (offset >> z_bits) & (BY - 1)
        wx, gx = spline(frac_ref[0, rows, cols])
        wy, gy = spline(frac_ref[1, rows, cols])
        wz, gz = spline(frac_ref[2, rows, cols])
        for k in range(3):
            keep(WX + k, wx[k])
            keep(GX + k, gx[k])
            keep(NRM + k, norm_ref[k, rows, cols])
            keep(WZ + k, wz[k])
            keep(GZ + k, gz[k])
        keep(WGT, weight_ref[rows, cols])
        at = [cell_y == m for m in range(BY)]
        for y in range(HALO_Y):
            taps = [k for k in range(3) if 0 <= y - k < BY]
            keep(YW + y, pick([at[y - k] for k in taps], [wy[k] for k in taps]))
            keep(YG + y, pick([at[y - k] for k in taps], [gy[k] for k in taps]))


def brick_table(capacity, slots, dest, count):
    tiles = dest.shape[1]
    across = jnp.broadcast_to(dest, (tiles, tiles))
    down = jnp.transpose(across)
    later = lax.broadcasted_iota(I32, (tiles, tiles), 0)
    sooner = lax.broadcasted_iota(I32, (tiles, tiles), 1)
    earlier = (across == down) & (sooner < later) & (sooner < count)
    rank = jnp.sum(jnp.where(earlier, 1, 0), axis=1, keepdims=True)
    tile = lax.broadcasted_iota(I32, (tiles, 1), 0)
    slot = jnp.where(tile < count, down[:, :1] * capacity + rank, -1)
    wanted = lax.broadcasted_iota(I32, (tiles, slots), 1)
    found = jnp.where(slot == wanted, jnp.broadcast_to(tile, (tiles, slots)), -1)
    return jnp.max(found, axis=0, keepdims=True)


def fused_kernel(
    capacity, n_slabs, n_columns, dest_hbm, count_hbm, off_hbm, frac_hbm, norm_hbm, weight_hbm, out_ref,
    dest, off, frac, norm, weight, table_v, table, chan, cell_z, grid,
    parts, core_in, mine, peer_in, ready, main_in, low_in, tail_low, tail_high,
    load_sem, core_sem, peer_sem, main_sem, low_sem, tail_sem,
):
    tiles, tile_len = off.shape
    halves = tile_len // LANES
    n_chips = n_columns // 2
    near = n_chips // 2
    last = n_slabs - 1
    me_x, me_y = lax.axis_index("gx"), lax.axis_index("yz")
    me_c, me_b = me_y // 2, lax.rem(me_y, 2)
    me_h, me_r = me_c // near, lax.rem(me_c, near)
    first_column = (n_columns // 2 - 1) * (1 - me_h)

    def slab_of(step):
        return lax.rem(me_x + 1 + step, n_slabs)

    def slab_at(hop):
        return lax.rem(me_x + hop + n_slabs, n_slabs)

    def column_at(hop):
        return 2 * lax.rem(me_c + hop, n_chips) + me_b

    def half_at(part):
        return lax.rem(me_h + 1 + part, 2)

    def place(part, turn):
        return lax.rem(me_r + turn, near)

    def hop_to(part, turn):
        return lax.rem(half_at(part) * near + place(part, turn) - me_c + n_chips, n_chips)

    loads = [
        pltpu.make_async_copy(dest_hbm, dest, load_sem.at[0]),
    ]
    span = tiles // CHUNKS
    chunks = []
    for n in range(CHUNKS):
        rows = pl.ds(n * span, span)
        base = 3 + 4 * n
        chunks.append([
            pltpu.make_async_copy(off_hbm.at[rows], off.at[rows], load_sem.at[base]),
            pltpu.make_async_copy(frac_hbm.at[:, rows], frac.at[:, rows], load_sem.at[base + 1]),
            pltpu.make_async_copy(norm_hbm.at[:, rows], norm.at[:, rows], load_sem.at[base + 2]),
            pltpu.make_async_copy(weight_hbm.at[rows], weight.at[rows], load_sem.at[base + 3]),
        ])
    for copy in loads + sum(chunks, []):
        copy.start()

    barrier = pltpu.get_barrier_semaphore()
    friends = [(me_x, me_y + 1 - 2 * me_b)]
    friends += [(slab_at(z), column_at(c)) for z in range(n_slabs) for c in range(n_chips) if z or c]
    for friend in friends:
        pl.semaphore_signal(barrier, inc=1, device_id=friend, device_id_type=MESH)

    grid[...] = jnp.zeros_like(grid)

    for copy in loads:
        copy.wait()
    table_v[...] = brick_table(capacity, table_v.shape[1], dest[...], count_hbm[0])

    def prepare_rows(step, _):
        prepare(pl.ds(pl.multiple_of(step * SUB, SUB), SUB), off, frac, norm, weight, chan, cell_z)
        return 0

    table_copy = pltpu.make_async_copy(table_v, table, load_sem.at[2])
    lead = 1
    for n in range(CHUNKS):
        for copy in chunks[n]:
            copy.wait()
        begin, end = n * span // SUB, (n + 1) * span // SUB
        if n == 0:
            lax.fori_loop(begin, begin + lead, prepare_rows, 0)
            table_copy.start()
            begin = begin + lead
        lax.fori_loop(begin, end, prepare_rows, 0)
    table_copy.wait()

    sub = lax.broadcasted_iota(I32, (SUB, LANES), 0)

    def layer_of(slab):
        return (sub + 4 * lax.rem(slab, 2)) & (SUB - 1)

    def brick_sum(step, column):
        slab = slab_of(step)
        brick = slab * n_columns + column
        layer = layer_of(slab)
        outside = ((layer == 0) & (slab == 0)) | ((layer == HALO_X - 1) & (slab == last))
        layer = jnp.where(outside, -SUB, layer).astype(F32)
        out = None
        for c in range(capacity):
            lefts, rights = [], []
            entry = table[0, brick * capacity + c]
            away = jnp.where(entry >= 0, 0.0, 8.0 * SUB)
            tile = jnp.minimum(jnp.maximum(entry, 0), tiles - 1)
            for half in range(halves):
                left, right = [[], [], []], [[], []]

                def row(n):
                    return jnp.broadcast_to(chan[half, n, pl.ds(tile, 1), :], (SUB, LANES))

                gap = layer - (row(CX) + away)
                hit = [gap == float(k) for k in range(3)]
                wx = pick(hit, [row(WX + k) for k in range(3)])
                gx = pick(hit, [row(GX + k) for k in range(3)])
                first, second = gx * row(NRM), wx * row(NRM + 1)
                third, plain = twice(wx * row(NRM + 2)), twice(wx * row(WGT))
                for m in range(HALO_Y // 2):
                    wy = [row(YW + 2 * m), row(YW + 2 * m + 1)]
                    gy = [row(YG + 2 * m), row(YG + 2 * m + 1)]
                    both = pair_up(first * wy[0] + second * gy[0], first * wy[1] + second * gy[1])
                    wide = pair_up(wy[0], wy[1])
                    left[0].append(both)
                    left[1].append(plain * wide)
                    left[2].append(third * wide)
                z = jnp.broadcast_to(cell_z[half, pl.ds(tile, 1), :], (SUB, LANES))
                tap = (sub - z + 1) & (SUB - 1)
                hit = [tap == k for k in range(3)]
                value = twice(pick(hit, [row(WZ + k) for k in range(3)]))
                slope = twice(pick(hit, [row(GZ + k) for k in range(3)]))
                home = ((z - 1 + tap) >> 3).astype(F32)
                home = pair_up(home, home - 1.0)
                zero = jnp.zeros_like(value)
                for m in range(BZ // (2 * SUB)):
                    here = home == jnp.bfloat16(2 * m)
                    right[0].append(jnp.where(here, value, zero))
                    right[1].append(jnp.where(here, slope, zero))
                lefts.append(jnp.concatenate(sum(left, []), axis=0))
                rights.append(jnp.concatenate(sum(right, []), axis=0))
            dims = (((1,), (1,)), ((), ()))
            more = lax.dot_general(
                jnp.concatenate(lefts, axis=1), jnp.concatenate(rights, axis=1), dims, preferred_element_type=F32
            )
            out = more if out is None else out + more
        return out

    def add_brick(step, k):
        column = lax.rem(first_column + k, n_columns)
        out = brick_sum(step, column)
        rhs = out[:ROWS, :BZ] + out[2 * ROWS :, BZ:]
        screen = out[ROWS : 2 * ROWS, :BZ]
        carried = (layer_of(slab_of(step)) < 2) & (step > 0)
        below = carried | (column > 0) if k > 0 else carried
        above = carried | (first_column > 0) if k == n_columns - 1 else carried
        for f, field in enumerate((rhs, screen)):
            for y in range(HALO_Y):
                at = pl.ds(pl.multiple_of((column * BY + y) * SUB, SUB), SUB)
                keep = below if y < 2 else above if y >= BY else carried
                old = jnp.where(keep, grid[f, at, :], 0.0)
                grid[f, at, :] = field[y * SUB : (y + 1) * SUB] + old

    def depth(j):
        return HALO_X if isinstance(j, int) and j == last else BX

    def core_copy(j, part):
        layers = pl.ds(0, depth(j))
        return pltpu.make_async_remote_copy(
            src_ref=parts.at[j, part, 1 - me_b, :, layers],
            dst_ref=core_in.at[j, part, :, layers],
            send_sem=core_sem.at[0, j, part],
            recv_sem=core_sem.at[1, j, part],
            device_id=(me_x, me_y + 1 - 2 * me_b),
            device_id_type=MESH,
        )

    def peer_copy(j, part, turn):
        hop = hop_to(part, turn)
        return pltpu.make_async_remote_copy(
            src_ref=mine.at[j, part, place(part, turn), pl.ds(depth(j) - BX - (depth(j) > BX), BX)],
            dst_ref=peer_in.at[j, hop],
            send_sem=peer_sem.at[0, j, hop],
            recv_sem=peer_sem.at[1, j, hop],
            device_id=(me_x, column_at(hop)),
            device_id_type=MESH,
        )

    peers = [(part, turn) for part in range(2) for turn in range(near) if (part, turn) != (1, 0)]

    def main_copy(j):
        return pltpu.make_async_remote_copy(
            src_ref=ready.at[j, pl.ds(1, BX - 1)],
            dst_ref=main_in.at[j],
            send_sem=main_sem.at[0, j],
            recv_sem=main_sem.at[1, j],
            device_id=(slab_at(1 + j), me_y),
            device_id_type=MESH,
        )

    def low_copy(j):
        return pltpu.make_async_remote_copy(
            src_ref=ready.at[j, 0],
            dst_ref=low_in.at[j],
            send_sem=low_sem.at[0, j],
            recv_sem=low_sem.at[1, j],
            device_id=(slab_at(j), me_y),
            device_id_type=MESH,
        )

    def tail_copy(side, part, turn):
        layer, target, to = ((0, tail_low, -1), (HALO_X - 1, tail_high, 1))[side]
        hop = hop_to(part, turn)
        return pltpu.make_async_remote_copy(
            src_ref=mine.at[last, part, place(part, turn), layer],
            dst_ref=target.at[hop],
            send_sem=tail_sem.at[0, side, hop],
            recv_sem=tail_sem.at[1, side, hop],
            device_id=(slab_at(to), column_at(hop)),
            device_id_type=MESH,
        )

    def share(j, part):
        start = 4 * lax.rem(slab_of(j), 2)
        base = half_at(part) * (n_columns // 2)
        for layer in range(depth(j)):
            at = lax.rem(start + layer, SUB)
            for k in range(n_columns // 2):
                for f in range(2):
                    rows = pl.ds(((base + k) * BY + 1) * SUB + at, BY, stride=SUB)
                    parts[j, part, k % 2, k // 2, layer, f] = grid[f, rows, :]
        core_copy(j, part).start()

    def spread(j, part):
        core_copy(j, part).wait()
        for chip in range(near):
            for layer in range(depth(j)):
                mine[j, part, chip, layer] = parts[j, part, me_b, chip, layer] + core_in[j, part, chip, layer]
        for turn in range(part, near):
            peer_copy(j, part, turn).start()
        if depth(j) > BX:
            for turn in range(near):
                tail_copy(0, part, turn).start()

            @pl.when(me_x < last)
            def _():
                for turn in range(near):
                    tail_copy(1, part, turn).start()

    def forward(j):
        for peer in peers:
            peer_copy(j, *peer).wait()
        for layer in range(BX):
            total = mine[j, 1, me_r, layer]
            for hop in range(1, n_chips):
                total = total + peer_in[j, hop, layer]
            ready[j, layer] = total
        main_copy(j).start()
        if j > 0:
            low_copy(j).start()

    split = n_columns // 2 + 1

    def early_step(step, _):
        for k in range(n_columns):
            add_brick(step, k)

        @pl.when(step == 0)
        def _():
            pl.semaphore_wait(barrier, len(friends))

        @pl.when(step > 0)
        def _():
            for part in range(2):
                spread(step - 1, part)

        for part in range(2):
            share(step, part)
        return 0

    lax.fori_loop(0, last - 1, early_step, 0)
    for step in (last - 1, last):
        for k in range(split):
            add_brick(step, k)
        if step < last:
            spread(step - 1, 0)
        spread(step - 1, 1)
        if step == last:
            for j in range(last - 2):
                forward(j)
        share(step, 0)
        for k in range(split, n_columns):
            add_brick(step, k)
        share(step, 1)
        spread(step, 0)
    for j in range(max(0, last - 2), last - 1):
        forward(j)
    spread(last, 1)
    forward(last - 1)
    for j in range(last):
        main_copy(j).wait()
        if j > 0:
            low_copy(j).wait()
    for peer in peers:
        peer_copy(last, *peer).wait()
    ends = [(part, turn) for part in range(2) for turn in range(near)]
    for end in ends:
        tail_copy(0, *end).wait()
    for layer in range(BX):
        total = mine[last, 1, me_r, layer + 1]
        for hop in range(1, n_chips):
            total = total + peer_in[last, hop, layer]
        if layer < BX - 1:
            for j in range(last):
                total = total + main_in[j, layer]
        else:
            total = total + ready[0, 0]
            for j in range(1, last):
                total = total + low_in[j]
            for hop in range(n_chips):
                total = total + tail_low[hop]
        for f in range(2):
            out_ref[f, layer] = total[f]

    @pl.when(me_x < last)
    def _():
        for end in ends:
            tail_copy(1, *end).wait_send()

    @pl.when(me_x > 0)
    def _():
        for end in ends:
            tail_copy(1, *end).wait_recv()
        for f in range(2):
            total = out_ref[f, 0]
            for hop in range(n_chips):
                total = total + tail_high[hop, f]
            out_ref[f, 0] = total


def hbm(array):
    return pltpu.with_memory_space_constraint(array, pltpu.HBM)


def fused(capacity, n_slabs, n_columns, dest, count, off, frac, norm, weight):
    tiles, tile_len = off.shape
    slots = n_slabs * n_columns * capacity
    n_chips = n_columns // 2
    block = (2, BY, BZ)
    dma = pltpu.SemaphoreType.DMA
    near = n_chips // 2
    return pl.pallas_call(
        functools.partial(fused_kernel, capacity, n_slabs, n_columns),
        out_shape=jax.ShapeDtypeStruct((2, BX, BY, BZ), F32),
        in_specs=[pl.BlockSpec(memory_space=pltpu.HBM), pl.BlockSpec(memory_space=pltpu.SMEM)] + [pl.BlockSpec(memory_space=pltpu.HBM)] * 4,
        out_specs=pl.BlockSpec(memory_space=pltpu.VMEM),
        scratch_shapes=[
            pltpu.VMEM((1, tiles), I32),
            pltpu.VMEM((tiles, tile_len), I32),
            pltpu.VMEM((3, tiles, tile_len), F32),
            pltpu.VMEM((3, tiles, tile_len), F32),
            pltpu.VMEM((tiles, tile_len), F32),
            pltpu.VMEM((1, slots), I32),
            pltpu.SMEM((1, slots), I32),
            pltpu.VMEM((tile_len // LANES, CHANNELS, tiles + SUB, LANES), F32),
            pltpu.VMEM((tile_len // LANES, tiles, LANES), I32),
            pltpu.VMEM((2, (n_columns * BY + 2) * SUB, BZ), F32),
            pltpu.VMEM((n_slabs, 2, 2, near, HALO_X) + block, F32),
            pltpu.VMEM((n_slabs, 2, near, HALO_X) + block, F32),
            pltpu.VMEM((n_slabs, 2, near, HALO_X) + block, F32),
            pltpu.VMEM((n_slabs, n_chips, BX) + block, F32),
            pltpu.VMEM((n_slabs, BX) + block, F32),
            pltpu.VMEM((n_slabs, BX - 1) + block, F32),
            pltpu.VMEM((n_slabs,) + block, F32),
            pltpu.VMEM((n_chips,) + block, F32),
            pltpu.VMEM((n_chips,) + block, F32),
            dma((3 + 4 * CHUNKS,)),
            dma((2, n_slabs, 2)),
            dma((2, n_slabs, n_chips)),
            dma((2, n_slabs)),
            dma((2, n_slabs)),
            dma((2, 2, n_chips)),
        ],
        compiler_params=pltpu.CompilerParams(collective_id=0, has_side_effects=True, vmem_limit_bytes=32 << 20),
        name="fused",
    )(hbm(dest), count, hbm(off), hbm(frac), hbm(norm), hbm(weight))


def shards(brick_ids, voxel_offset, fractions, normals, point_weight, tile_count):
    n_slabs = lax.axis_size("gx")
    n_columns = lax.axis_size("yz")
    devices = n_slabs * n_columns
    tiles_here = brick_ids.shape[0]
    capacity = max(2, (tiles_here + devices - 1) // devices)
    both = fused(
        capacity, n_slabs, n_columns, brick_ids.reshape(1, tiles_here), tile_count, voxel_offset,
        jnp.transpose(fractions, (1, 0, 2)), jnp.transpose(normals, (1, 0, 2)), point_weight,
    )
    return (both[0], both[1])


def solution(mesh):
    return jax.shard_map(
        shards,
        mesh=mesh,
        in_specs=(
            P(("gx", "yz"), None),
            P(("gx", "yz"), None),
            P(("gx", "yz"), None, None),
            P(("gx", "yz"), None, None),
            P(("gx", "yz"), None),
            P(("gx", "yz")),
        ),
        out_specs=(P("gx", "yz", None), P("gx", "yz", None)),
        check_vma=False,
    )
```

```python
import functools

import jax
import jax.numpy as jnp
from jax import lax
from jax.experimental import pallas as pl
from jax.experimental.pallas import tpu as pltpu
from jax.sharding import PartitionSpec as P

BX = 4
BY = 8
BZ = 128
MESH = pl.DeviceIdType.MESH
F32, BF16, I32 = jnp.float32, jnp.bfloat16, jnp.int32
LANES = 128
SUB = 8
HALO_X = BX + 2
HALO_Y = BY + 2
ROWS = HALO_Y * SUB
CHUNKS = 2
CX, WX, GX, NRM, WGT, YW, YG, WZ, GZ = 0, 1, 4, 7, 10, 11, 11 + HALO_Y, 11 + 2 * HALO_Y, 14 + 2 * HALO_Y
CHANNELS = 17 + 2 * HALO_Y


def spline(frac):
    weights = [0.5 * (1.0 - frac) ** 2, 0.75 - (frac - 0.5) ** 2, 0.5 * frac * frac]
    slopes = [frac - 1.0, 1.0 - 2.0 * frac, frac]
    return (weights, slopes)


def pick(masks, values):
    out = jnp.zeros_like(values[0])
    for mask, value in zip(masks, values):
        out = jnp.where(mask, value, out)
    return out


def twice(value):
    return jnp.concatenate([value, value], axis=0).astype(BF16)


def pair_up(upper, lower):
    return jnp.concatenate([upper, lower], axis=0).astype(BF16)


def prepare(rows, off_ref, frac_ref, norm_ref, weight_ref, chan, cell_z):
    z_bits, y_bits = BZ.bit_length() - 1, BY.bit_length() - 1
    for half in range(chan.shape[0]):
        cols = pl.ds(half * LANES, LANES)

        def keep(n, value):
            chan[half, n, rows, :] = value

        offset = off_ref[rows, cols]
        keep(CX, (offset >> (z_bits + y_bits)).astype(F32))
        cell_z[half, rows, :] = offset & (BZ - 1)
        cell_y = (offset >> z_bits) & (BY - 1)
        wx, gx = spline(frac_ref[0, rows, cols])
        wy, gy = spline(frac_ref[1, rows, cols])
        wz, gz = spline(frac_ref[2, rows, cols])
        for k in range(3):
            keep(WX + k, wx[k])
            keep(GX + k, gx[k])
            keep(NRM + k, norm_ref[k, rows, cols])
            keep(WZ + k, wz[k])
            keep(GZ + k, gz[k])
        keep(WGT, weight_ref[rows, cols])
        at = [cell_y == m for m in range(BY)]
        for y in range(HALO_Y):
            taps = [k for k in range(3) if 0 <= y - k < BY]
            keep(YW + y, pick([at[y - k] for k in taps], [wy[k] for k in taps]))
            keep(YG + y, pick([at[y - k] for k in taps], [gy[k] for k in taps]))


def brick_table(capacity, slots, dest, count):
    tiles = dest.shape[1]
    across = jnp.broadcast_to(dest, (tiles, tiles))
    down = jnp.transpose(across)
    later = lax.broadcasted_iota(I32, (tiles, tiles), 0)
    sooner = lax.broadcasted_iota(I32, (tiles, tiles), 1)
    earlier = (across == down) & (sooner < later) & (sooner < count)
    rank = jnp.sum(jnp.where(earlier, 1, 0), axis=1, keepdims=True)
    tile = lax.broadcasted_iota(I32, (tiles, 1), 0)
    slot = jnp.where(tile < count, down[:, :1] * capacity + rank, -1)
    wanted = lax.broadcasted_iota(I32, (tiles, slots), 1)
    found = jnp.where(slot == wanted, jnp.broadcast_to(tile, (tiles, slots)), tiles)
    return jnp.min(found, axis=0, keepdims=True)


def fused_kernel(
    capacity, n_slabs, n_columns, dest_hbm, count_hbm, off_hbm, frac_hbm, norm_hbm, weight_hbm, out_ref,
    dest, off, frac, norm, weight, table_v, table, chan, cell_z, grid,
    parts, core_in, mine, peer_in, ready, main_in, low_in, tail_low, tail_high,
    load_sem, core_sem, peer_sem, main_sem, low_sem, tail_sem,
):
    tiles, tile_len = off.shape
    halves = tile_len // LANES
    n_chips = n_columns // 2
    near = n_chips // 2
    last = n_slabs - 1
    me_x, me_y = lax.axis_index("gx"), lax.axis_index("yz")
    me_c, me_b = me_y // 2, lax.rem(me_y, 2)
    me_h, me_r = me_c // near, lax.rem(me_c, near)
    first_column = (n_columns // 2 - 1) * (1 - me_h)

    def slab_of(step):
        return lax.rem(me_x + 1 + step, n_slabs)

    def slab_at(hop):
        return lax.rem(me_x + hop + n_slabs, n_slabs)

    def column_at(hop):
        return 2 * lax.rem(me_c + hop, n_chips) + me_b

    def half_at(part):
        return lax.rem(me_h + 1 + part, 2)

    def place(part, turn):
        return lax.rem(me_r + turn, near)

    def hop_to(part, turn):
        return lax.rem(half_at(part) * near + place(part, turn) - me_c + n_chips, n_chips)

    loads = [
        pltpu.make_async_copy(dest_hbm, dest, load_sem.at[0]),
    ]
    span = tiles // CHUNKS
    chunks = []
    for n in range(CHUNKS):
        rows = pl.ds(n * span, span)
        base = 3 + 4 * n
        chunks.append([
            pltpu.make_async_copy(off_hbm.at[rows], off.at[rows], load_sem.at[base]),
            pltpu.make_async_copy(frac_hbm.at[:, rows], frac.at[:, rows], load_sem.at[base + 1]),
            pltpu.make_async_copy(norm_hbm.at[:, rows], norm.at[:, rows], load_sem.at[base + 2]),
            pltpu.make_async_copy(weight_hbm.at[rows], weight.at[rows], load_sem.at[base + 3]),
        ])
    for copy in loads + sum(chunks, []):
        copy.start()

    barrier = pltpu.get_barrier_semaphore()
    friends = [(me_x, me_y + 1 - 2 * me_b)]
    friends += [(slab_at(z), column_at(c)) for z in range(n_slabs) for c in range(n_chips) if z or c]
    for friend in friends:
        pl.semaphore_signal(barrier, inc=1, device_id=friend, device_id_type=MESH)

    grid[...] = jnp.zeros_like(grid)
    blank = pl.ds(tiles, SUB)
    for half in range(halves):
        for n in range(CHANNELS):
            chan[half, n, blank, :] = jnp.full((SUB, LANES), 8.0 * SUB if n == CX else 0.0, F32)
        cell_z[half, blank, :] = jnp.zeros((SUB, LANES), I32)


    for copy in loads:
        copy.wait()
    table_v[...] = brick_table(capacity, table_v.shape[1], dest[...], count_hbm[0])

    def prepare_rows(step, _):
        prepare(pl.ds(pl.multiple_of(step * SUB, SUB), SUB), off, frac, norm, weight, chan, cell_z)
        return 0

    table_copy = pltpu.make_async_copy(table_v, table, load_sem.at[2])
    lead = 1
    for n in range(CHUNKS):
        for copy in chunks[n]:
            copy.wait()
        begin, end = n * span // SUB, (n + 1) * span // SUB
        if n == 0:
            lax.fori_loop(begin, begin + lead, prepare_rows, 0)
            table_copy.start()
            begin = begin + lead
        lax.fori_loop(begin, end, prepare_rows, 0)
    table_copy.wait()

    sub = lax.broadcasted_iota(I32, (SUB, LANES), 0)

    ahead = sub + 1

    def layer_of(slab):
        return (sub + 4 * lax.rem(slab, 2)) & (SUB - 1)

    def brick_sum(step, column):
        slab = slab_of(step)
        brick = slab * n_columns + column
        layer = layer_of(slab)
        outside = ((layer == 0) & (slab == 0)) | ((layer == HALO_X - 1) & (slab == last))
        layer = jnp.where(outside, -SUB, layer).astype(F32)
        out = None
        for c in range(capacity):
            lefts, rights = [], []
            entry = table[0, brick * capacity + c]
            tile = jnp.minimum(jnp.maximum(entry, 0), tiles)
            for half in range(halves):
                left, right = [[], [], []], [[], []]

                def row(n):
                    return jnp.broadcast_to(chan[half, n, pl.ds(tile, 1), :], (SUB, LANES))

                gap = layer - row(CX)
                hit = [gap == float(k) for k in range(3)]
                wx = pick(hit, [row(WX + k) for k in range(3)])
                gx = pick(hit, [row(GX + k) for k in range(3)])
                first, second = gx * row(NRM), wx * row(NRM + 1)
                third, plain = twice(wx * row(NRM + 2)), twice(wx * row(WGT))
                for m in range(HALO_Y // 2):
                    wy = [row(YW + 2 * m), row(YW + 2 * m + 1)]
                    gy = [row(YG + 2 * m), row(YG + 2 * m + 1)]
                    both = pair_up(first * wy[0] + second * gy[0], first * wy[1] + second * gy[1])
                    wide = pair_up(wy[0], wy[1])
                    left[0].append(both)
                    left[1].append(plain * wide)
                    left[2].append(third * wide)
                z = jnp.broadcast_to(cell_z[half, pl.ds(tile, 1), :], (SUB, LANES))
                lag = ahead - z
                tap = lag & (SUB - 1)
                hit = [tap == k for k in range(3)]
                value = twice(pick(hit, [row(WZ + k) for k in range(3)]))
                slope = twice(pick(hit, [row(GZ + k) for k in range(3)]))
                home = (tap - lag).astype(F32)
                home = pair_up(home, home - SUB)
                zero = jnp.zeros_like(value)
                for m in range(BZ // (2 * SUB)):
                    here = home == jnp.bfloat16(2 * SUB * m)
                    right[0].append(jnp.where(here, value, zero))
                    right[1].append(jnp.where(here, slope, zero))
                lefts.append(jnp.concatenate(sum(left, []), axis=0))
                rights.append(jnp.concatenate(sum(right, []), axis=0))
            dims = (((1,), (1,)), ((), ()))
            more = lax.dot_general(
                jnp.concatenate(lefts, axis=1), jnp.concatenate(rights, axis=1), dims, preferred_element_type=F32
            )
            out = more if out is None else out + more
        return out

    def add_brick(step, k):
        column = lax.rem(first_column + k, n_columns)
        out = brick_sum(step, column)
        rhs = out[:ROWS, :BZ] + out[2 * ROWS :, BZ:]
        screen = out[ROWS : 2 * ROWS, :BZ]
        carried = (layer_of(slab_of(step)) < 2) & (step > 0)
        below = carried | (column > 0) if k > 0 else carried
        above = carried | (first_column > 0) if k == n_columns - 1 else carried
        for f, field in enumerate((rhs, screen)):
            for y in range(HALO_Y):
                at = pl.ds(pl.multiple_of((column * BY + y) * SUB, SUB), SUB)
                keep = below if y < 2 else above if y >= BY else carried
                old = jnp.where(keep, grid[f, at, :], 0.0)
                grid[f, at, :] = field[y * SUB : (y + 1) * SUB] + old

    def depth(j):
        return HALO_X if isinstance(j, int) and j == last else BX

    def core_copy(j, part):
        layers = pl.ds(0, depth(j))
        return pltpu.make_async_remote_copy(
            src_ref=parts.at[j, part, 1 - me_b, :, layers],
            dst_ref=core_in.at[j, part, :, layers],
            send_sem=core_sem.at[0, j, part],
            recv_sem=core_sem.at[1, j, part],
            device_id=(me_x, me_y + 1 - 2 * me_b),
            device_id_type=MESH,
        )

    def peer_copy(j, part, turn):
        hop = hop_to(part, turn)
        return pltpu.make_async_remote_copy(
            src_ref=mine.at[j, part, place(part, turn), pl.ds(depth(j) - BX - (depth(j) > BX), BX)],
            dst_ref=peer_in.at[j, hop],
            send_sem=peer_sem.at[0, j, hop],
            recv_sem=peer_sem.at[1, j, hop],
            device_id=(me_x, column_at(hop)),
            device_id_type=MESH,
        )

    peers = [(part, turn) for part in range(2) for turn in range(near) if (part, turn) != (1, 0)]

    def main_copy(j):
        return pltpu.make_async_remote_copy(
            src_ref=ready.at[j, pl.ds(1, BX - 1)],
            dst_ref=main_in.at[j],
            send_sem=main_sem.at[0, j],
            recv_sem=main_sem.at[1, j],
            device_id=(slab_at(1 + j), me_y),
            device_id_type=MESH,
        )

    def low_copy(j):
        return pltpu.make_async_remote_copy(
            src_ref=ready.at[j, 0],
            dst_ref=low_in.at[j],
            send_sem=low_sem.at[0, j],
            recv_sem=low_sem.at[1, j],
            device_id=(slab_at(j), me_y),
            device_id_type=MESH,
        )

    def tail_copy(side, part, turn):
        layer, target, to = ((0, tail_low, -1), (HALO_X - 1, tail_high, 1))[side]
        hop = hop_to(part, turn)
        return pltpu.make_async_remote_copy(
            src_ref=mine.at[last, part, place(part, turn), layer],
            dst_ref=target.at[hop],
            send_sem=tail_sem.at[0, side, hop],
            recv_sem=tail_sem.at[1, side, hop],
            device_id=(slab_at(to), column_at(hop)),
            device_id_type=MESH,
        )

    def share(j, part):
        start = 4 * lax.rem(slab_of(j), 2)
        base = half_at(part) * (n_columns // 2)
        for layer in range(depth(j)):
            at = lax.rem(start + layer, SUB)
            for k in range(n_columns // 2):
                for f in range(2):
                    rows = pl.ds(((base + k) * BY + 1) * SUB + at, BY, stride=SUB)
                    parts[j, part, k % 2, k // 2, layer, f] = grid[f, rows, :]
        core_copy(j, part).start()

    def spread(j, part):
        core_copy(j, part).wait()
        for chip in range(near):
            for layer in range(depth(j)):
                mine[j, part, chip, layer] = parts[j, part, me_b, chip, layer] + core_in[j, part, chip, layer]
        for turn in range(part, near):
            peer_copy(j, part, turn).start()
        if depth(j) > BX:
            for turn in range(near):
                tail_copy(0, part, turn).start()

            @pl.when(me_x < last)
            def _():
                for turn in range(near):
                    tail_copy(1, part, turn).start()

    def forward(j):
        for peer in peers:
            peer_copy(j, *peer).wait()
        for layer in range(BX):
            total = mine[j, 1, me_r, layer]
            for hop in range(1, n_chips):
                total = total + peer_in[j, hop, layer]
            ready[j, layer] = total
        main_copy(j).start()
        if j > 0:
            low_copy(j).start()

    split = n_columns // 2 + 1

    def early_step(step, _):
        for k in range(n_columns):
            add_brick(step, k)

        @pl.when(step == 0)
        def _():
            pl.semaphore_wait(barrier, len(friends))

        @pl.when(step > 0)
        def _():
            for part in range(2):
                spread(step - 1, part)

        for part in range(2):
            share(step, part)
        return 0

    lax.fori_loop(0, last - 1, early_step, 0)
    for step in (last - 1, last):
        for k in range(split):
            add_brick(step, k)
        share(step, 0)
        if step < last:
            spread(step - 1, 0)
        spread(step - 1, 1)
        if step == last:
            for j in range(last - 2):
                forward(j)
        for k in range(split, n_columns):
            add_brick(step, k)
        share(step, 1)
        spread(step, 0)
    for j in range(max(0, last - 2), last - 1):
        forward(j)
    spread(last, 1)
    forward(last - 1)
    for j in range(last):
        main_copy(j).wait()
        if j > 0:
            low_copy(j).wait()
    for peer in peers:
        peer_copy(last, *peer).wait()
    ends = [(part, turn) for part in range(2) for turn in range(near)]
    for end in ends:
        tail_copy(0, *end).wait()
    for layer in range(BX):
        total = mine[last, 1, me_r, layer + 1]
        for hop in range(1, n_chips):
            total = total + peer_in[last, hop, layer]
        if layer < BX - 1:
            for j in range(last):
                total = total + main_in[j, layer]
        else:
            total = total + ready[0, 0]
            for j in range(1, last):
                total = total + low_in[j]
            for hop in range(n_chips):
                total = total + tail_low[hop]
        for f in range(2):
            out_ref[f, layer] = total[f]

    @pl.when(me_x < last)
    def _():
        for end in ends:
            tail_copy(1, *end).wait_send()

    @pl.when(me_x > 0)
    def _():
        for end in ends:
            tail_copy(1, *end).wait_recv()
        for f in range(2):
            total = out_ref[f, 0]
            for hop in range(n_chips):
                total = total + tail_high[hop, f]
            out_ref[f, 0] = total


def hbm(array):
    return pltpu.with_memory_space_constraint(array, pltpu.HBM)


def fused(capacity, n_slabs, n_columns, dest, count, off, frac, norm, weight):
    tiles, tile_len = off.shape
    slots = n_slabs * n_columns * capacity
    n_chips = n_columns // 2
    block = (2, BY, BZ)
    dma = pltpu.SemaphoreType.DMA
    near = n_chips // 2
    return pl.pallas_call(
        functools.partial(fused_kernel, capacity, n_slabs, n_columns),
        out_shape=jax.ShapeDtypeStruct((2, BX, BY, BZ), F32),
        in_specs=[pl.BlockSpec(memory_space=pltpu.HBM), pl.BlockSpec(memory_space=pltpu.SMEM)] + [pl.BlockSpec(memory_space=pltpu.HBM)] * 4,
        out_specs=pl.BlockSpec(memory_space=pltpu.VMEM),
        scratch_shapes=[
            pltpu.VMEM((1, tiles), I32),
            pltpu.VMEM((tiles, tile_len), I32),
            pltpu.VMEM((3, tiles, tile_len), F32),
            pltpu.VMEM((3, tiles, tile_len), F32),
            pltpu.VMEM((tiles, tile_len), F32),
            pltpu.VMEM((1, slots), I32),
            pltpu.SMEM((1, slots), I32),
            pltpu.VMEM((tile_len // LANES, CHANNELS, tiles + SUB, LANES), F32),
            pltpu.VMEM((tile_len // LANES, tiles + SUB, LANES), I32),
            pltpu.VMEM((2, (n_columns * BY + 2) * SUB, BZ), F32),
            pltpu.VMEM((n_slabs, 2, 2, near, HALO_X) + block, F32),
            pltpu.VMEM((n_slabs, 2, near, HALO_X) + block, F32),
            pltpu.VMEM((n_slabs, 2, near, HALO_X) + block, F32),
            pltpu.VMEM((n_slabs, n_chips, BX) + block, F32),
            pltpu.VMEM((n_slabs, BX) + block, F32),
            pltpu.VMEM((n_slabs, BX - 1) + block, F32),
            pltpu.VMEM((n_slabs,) + block, F32),
            pltpu.VMEM((n_chips,) + block, F32),
            pltpu.VMEM((n_chips,) + block, F32),
            dma((3 + 4 * CHUNKS,)),
            dma((2, n_slabs, 2)),
            dma((2, n_slabs, n_chips)),
            dma((2, n_slabs)),
            dma((2, n_slabs)),
            dma((2, 2, n_chips)),
        ],
        compiler_params=pltpu.CompilerParams(collective_id=0, has_side_effects=True, vmem_limit_bytes=32 << 20),
        name="fused",
    )(hbm(dest), count, hbm(off), hbm(frac), hbm(norm), hbm(weight))


def shards(brick_ids, voxel_offset, fractions, normals, point_weight, tile_count):
    n_slabs = lax.axis_size("gx")
    n_columns = lax.axis_size("yz")
    devices = n_slabs * n_columns
    tiles_here = brick_ids.shape[0]
    capacity = max(2, (tiles_here + devices - 1) // devices)
    both = fused(
        capacity, n_slabs, n_columns, brick_ids.reshape(1, tiles_here), tile_count, voxel_offset,
        jnp.transpose(fractions, (1, 0, 2)), jnp.transpose(normals, (1, 0, 2)), point_weight,
    )
    return (both[0], both[1])


def solution(mesh):
    return jax.shard_map(
        shards,
        mesh=mesh,
        in_specs=(
            P(("gx", "yz"), None),
            P(("gx", "yz"), None),
            P(("gx", "yz"), None, None),
            P(("gx", "yz"), None, None),
            P(("gx", "yz"), None),
            P(("gx", "yz")),
        ),
        out_specs=(P("gx", "yz", None), P("gx", "yz", None)),
        check_vma=False,
    )
```
